256 devices in a mesh: grp: 8 (over y, core), head: 32 (over z, x).
Axes of the slice: x: 4, y: 4, z: 8, core: 2. Of those that a mesh axis runs over, the one named last changes fastest.
Arguments:
- hidden_in: bfloat16 [192, 4096], P('grp', 'head'), may hold values from -6 to 6
- attention_gain: float32 [4096], replicated, may hold values from 0.1 to 1.9
- w_query: bfloat16 [4096, 4096], P(None, 'head'), may hold values from -0.09375 to 0.09375
- w_key_value: bfloat16 [2, 4096, 4096], P(None, None, 'head'), as said below
- w_attention_out: bfloat16 [4096, 4096], P('head'), may hold values from -0.09375 to 0.09375
- past_cache: bfloat16 [2, 192, 32, 128, 128], P(None, 'grp', 'head'), may hold values from -2000 to 2000, as said below
- lengths: int32 [192], P('grp'), may hold values from 2 to 128, as said below
- mamba_gain: float32 [4096], replicated, may hold values from 0.1 to 1.9
- w_in: bfloat16 [2, 4096, 8192], P(None, None, 'head'), may hold values from -0.09375 to 0.09375
- filter_weight: float32 [4, 8192], P(None, 'head'), may hold values from -3 to 3
- filter_bias: float32 [8192], P('head'), may hold values from -1.8 to 1.8
- filter_state: float32 [192, 3, 8192], P('grp', None, 'head'), may hold values from -6 to 6
- w_select: bfloat16 [8192, 288], P('head'), may hold values from -0.0625 to 0.0625
- w_step: bfloat16 [256, 8192], P(None, 'head'), may hold values from -0.375 to 0.375
- step_bias: float32 [8192], P('head'), may hold values from -4 to -1
- log_rate: float32 [16, 8192], P(None, 'head'), may hold values from 0 to 2.77
- skip_gain: float32 [8192], P('head'), may hold values from 0.1 to 1.9
- scan_state: float32 [192, 16, 8192], P('grp', None, 'head'), may hold values from -6 to 6
- w_mamba_out: bfloat16 [8192, 4096], P('head'), may hold values from -0.0625 to 0.0625
- reward_terms: float32 [192, 128], P('grp', 'head'), may hold values from -60 to 60
- reward_mask: int32 [192, 128], P('grp', 'head'), may hold values 0 or 1
Outputs:
- hidden_out: bfloat16 [192, 4096], P('grp', 'head')
- new_key_value: bfloat16 [2, 192, 32, 128], P(None, 'grp', 'head')
- new_filter_state: float32 [192, 3, 8192], P('grp', None, 'head')
- new_scan_state: float32 [192, 16, 8192], P('grp', None, 'head')
- rewards: float32 [192], P('grp')
The draws below stay inside these ranges and needn't reach their ends.
Inputs may be any that keep to these rules, and one draw needn't show every extreme that they name: `w_key_value`: query heads that share a key-value head (4 of them in a row) hold equal copies. `past_cache`: query heads that share a key-value head (4 of them in a row) hold equal copies. `lengths`: the first sample's cache is full (128).
All inputs are finite; a program needn't handle non-finite values. No bound on the sum of `reward_mask` on one device may be relied on, other than what follows from the above.
Results may differ from the reference program's by a relative error of at most 0.012.
Values may be sent and summed in bfloat16 or wider, within the bound.
A program may use at most 64 MiB of HBM per device.

```python
import math
import jax
import jax.numpy as jnp
from jax import lax

D = 4096
HEADS = 32
KVH = 8
DH = 128
INNER = 8192
NSTATE = 16
CONV = 4
RANK = 256
CTX = 128
BATCH = 192


def draw_w_key_value(key, part):
    drawn = jax.random.normal(key, (2, D, KVH, DH), jnp.float32) * D ** (-0.5)
    copies = jnp.repeat(drawn, HEADS // KVH, axis=2)
    return copies.reshape(2, D, HEADS * DH).astype(jnp.bfloat16)


def draw_past_cache(key, part):
    base_key = jax.random.fold_in(key, 0)
    drawn = jnp.clip(jax.random.normal(base_key, (2, BATCH, KVH, CTX, DH), jnp.float32), -6.0, 6.0)
    return jnp.repeat(drawn, HEADS // KVH, axis=2).astype(jnp.bfloat16)


def draw_lengths(key, part):
    drawn = jax.random.randint(key, (BATCH,), 2, CTX + 1, dtype=jnp.int32)
    return drawn.at[0].set(CTX)


def draw_reward_terms(key, part):
    noise_key = jax.random.fold_in(key, 0)
    ramp = 1.0 + 2.0 * jnp.arange(CTX, dtype=jnp.float32) / (CTX - 1)
    noise = jnp.clip(jax.random.normal(noise_key, (BATCH, CTX), jnp.float32), -6.0, 6.0)
    return noise * ramp[None, :]


def plant(result, key, least, largest):
    shape = result.shape
    place = [jax.random.randint(jax.random.fold_in(key, axis), (), 0, shape[axis]) for axis in range(len(shape))]
    result = result.at[tuple(place)].set(least)
    longest = shape.index(max(shape))
    place[longest] = (place[longest] + 1) % shape[longest]
    return result.at[tuple(place)].set(largest)


def block_levels(own_key, extent, shards, low, high):
    def one(position, shards_of):
        steps = jax.random.uniform(jax.random.fold_in(jax.random.fold_in(own_key, 6), position), (shards_of,), jnp.float32, low / len(shards), high / len(shards))
        return jnp.repeat(jnp.exp(steps), extent[position] // shards_of).reshape((-1,) + (1,) * (len(extent) - position - 1))

    level = one(*shards[0])
    for cut in shards[1:]:
        level = level * one(*cut)
    return level


def bell_draw(stream_key, shape, width, limit, cuts=(), held_as=jnp.bfloat16):
    level = block_levels(stream_key, shape, cuts, -0.22, 0.18) if cuts else 1.0
    array = jax.random.normal(stream_key, shape, jnp.float32) * width * level
    return jnp.minimum(jnp.maximum(array, -limit), limit).astype(held_as)


def setup_inputs(seed: int = 0) -> dict:
    key_of = jax.random.split(jax.random.key(seed), 22)
    return {
        "hidden_in": bell_draw(key_of[0], (BATCH, D), 1.0, 6.0, ((0, 8), (1, 32))),
        "attention_gain": jnp.clip(1.0 + 0.18 * jax.random.normal(key_of[1], (D,), jnp.float32), 0.1, 1.9),
        "w_query": bell_draw(key_of[2], (D, HEADS * DH), D ** -0.5, 0.09375, ((1, 32),)),
        "w_key_value": draw_w_key_value(jax.random.fold_in(key_of[21], 71), 0),
        "w_attention_out": bell_draw(key_of[4], (HEADS * DH, D), (HEADS * DH) ** -0.5, 0.09375, ((0, 32),)),
        "past_cache": draw_past_cache(jax.random.fold_in(key_of[21], 71), 0),
        "lengths": draw_lengths(jax.random.fold_in(key_of[21], 71), 0),
        "mamba_gain": jnp.clip(1.0 + 0.18 * jax.random.normal(key_of[7], (D,), jnp.float32), 0.1, 1.9),
        "w_in": bell_draw(key_of[8], (2, D, INNER), D ** -0.5, 0.09375, ((2, 32),)),
        "filter_weight": bell_draw(key_of[9], (CONV, INNER), CONV ** -0.5, 3.0, ((1, 32),), jnp.float32),
        "filter_bias": bell_draw(key_of[10], (INNER,), 0.3, 1.8, ((0, 32),), jnp.float32),
        "filter_state": bell_draw(key_of[11], (BATCH, CONV - 1, INNER), 1.0, 6.0, ((0, 8), (2, 32)), jnp.float32),
        "w_select": bell_draw(key_of[12], (INNER, RANK + 2 * NSTATE), INNER ** -0.5, 0.0625, ((0, 32),)),
        "w_step": bell_draw(key_of[13], (RANK, INNER), RANK ** -0.5, 0.375, ((1, 32),)),
        "step_bias": jnp.clip(-4.0 + 3.0 * jax.random.uniform(key_of[14], (INNER,), jnp.float32) ** block_levels(key_of[14], (INNER,), ((0, 32),), -0.2, 0.2), -4.0, -1.0),
        "log_rate": jnp.clip(2.77 * jax.random.uniform(key_of[15], (NSTATE, INNER), jnp.float32) ** block_levels(key_of[15], (NSTATE, INNER), ((1, 32),), -0.2, 0.2), 0.0, 2.77),
        "skip_gain": jnp.clip(1.0 + 0.18 * jax.random.normal(key_of[16], (INNER,), jnp.float32), 0.1, 1.9),
        "scan_state": bell_draw(key_of[17], (BATCH, NSTATE, INNER), 1.0, 6.0, ((0, 8), (2, 32)), jnp.float32),
        "w_mamba_out": bell_draw(key_of[18], (INNER, D), INNER ** -0.5, 0.0625, ((0, 32),)),
        "reward_terms": draw_reward_terms(jax.random.fold_in(key_of[21], 71), 0),
        "reward_mask": plant((jax.random.randint(key_of[20], (BATCH, CTX), 0, 2) < 1).astype(jnp.int32), jax.random.fold_in(key_of[20], 1), 0, 1),
    }


EPS = 1e-06

def norm_rows(row_values, gain):
    values = row_values.astype(jnp.float32)
    factor = lax.rsqrt(lax.optimization_barrier(jnp.mean(values * values, axis=-1, keepdims=True)) + EPS)
    return (values * factor * gain).astype(jnp.bfloat16)

def attend_sample(query, cache, fresh, length):
    inv_root = 1.0 / math.sqrt(query.shape[-1])
    query_wide = query.astype(jnp.float32)
    scores = jnp.einsum('hd,htd->ht', query_wide, cache[0].astype(jnp.float32)) * inv_root
    positions = jnp.arange(cache.shape[2], dtype=jnp.int32)
    scores = jnp.where(positions[None, :] < length, scores, -jnp.inf)
    own_score = lax.optimization_barrier(jnp.sum(query_wide * fresh[0].astype(jnp.float32), axis=-1)) * inv_root
    row_max = jnp.maximum(lax.optimization_barrier(jnp.max(scores, axis=-1)), own_score)
    weights = jnp.exp(scores - row_max[:, None])
    own_weight = jnp.exp(own_score - row_max)
    denominator = lax.optimization_barrier(jnp.sum(weights, axis=-1)) + own_weight
    weights = (weights / denominator[:, None]).astype(jnp.bfloat16)
    own_weight = (own_weight / denominator).astype(jnp.bfloat16)
    blended = jnp.einsum('ht,htd->hd', weights.astype(jnp.float32), cache[1].astype(jnp.float32))
    blended = blended + own_weight.astype(jnp.float32)[:, None] * fresh[1].astype(jnp.float32)
    return blended.astype(jnp.bfloat16)

def reference(hidden_in, attention_gain, w_query, w_key_value, w_attention_out, past_cache, lengths, mamba_gain, w_in, filter_weight, filter_bias, filter_state, w_select, w_step, step_bias, log_rate, skip_gain, scan_state, w_mamba_out, reward_terms, reward_mask):
    normed = norm_rows(hidden_in, attention_gain)
    queries = jnp.dot(normed, w_query, preferred_element_type=jnp.float32).astype(jnp.bfloat16)
    queries = queries.reshape(BATCH, HEADS, DH)
    fresh_all = jnp.einsum('bd,kdc->kbc', normed.astype(jnp.float32), w_key_value.astype(jnp.float32))
    new_key_value = fresh_all.astype(jnp.bfloat16).reshape(2, BATCH, HEADS, DH)

    def one_sample(index):
        cache = lax.dynamic_index_in_dim(past_cache, index, 1, keepdims=False)
        fresh = lax.dynamic_index_in_dim(new_key_value, index, 1, keepdims=False)
        query = lax.dynamic_index_in_dim(queries, index, 0, keepdims=False)
        length = lax.dynamic_index_in_dim(lengths, index, 0, keepdims=False)
        return attend_sample(query, cache, fresh, length)
    attended = lax.map(one_sample, jnp.arange(BATCH, dtype=jnp.int32)).reshape(BATCH, HEADS * DH)
    head_terms = jnp.dot(attended, w_attention_out, preferred_element_type=jnp.float32)
    mixed = (hidden_in.astype(jnp.float32) + head_terms).astype(jnp.bfloat16)
    normed_two = norm_rows(mixed, mamba_gain)
    x_inner = jnp.dot(normed_two, w_in[0], preferred_element_type=jnp.float32)
    gate_part = jnp.dot(normed_two, w_in[1], preferred_element_type=jnp.float32)
    conv_sum = filter_bias + x_inner * filter_weight[CONV - 1]
    for tap_index in range(CONV - 1):
        conv_sum = conv_sum + filter_state[:, tap_index, :] * filter_weight[tap_index]
    conv_out = jax.nn.silu(conv_sum).astype(jnp.bfloat16)
    new_filter_state = jnp.concatenate([filter_state[:, 1:, :], x_inner[:, None, :]], axis=1)
    projected = jnp.dot(conv_out, w_select, preferred_element_type=jnp.float32)
    step_low = projected[:, :RANK].astype(jnp.bfloat16)
    b_input = projected[:, RANK:RANK + NSTATE]
    c_output = projected[:, RANK + NSTATE:]
    step_size = jax.nn.softplus(jnp.dot(step_low, w_step, preferred_element_type=jnp.float32) + step_bias)
    conv_value = conv_out.astype(jnp.float32)
    decay_rate = jnp.exp(-step_size[:, None, :] * jnp.exp(log_rate)[None, :, :])
    new_scan_state = decay_rate * scan_state + step_size[:, None, :] * b_input[:, :, None] * conv_value[:, None, :]
    scan_out = (lax.optimization_barrier(jnp.sum(c_output[:, :, None] * new_scan_state, axis=1)) + skip_gain * conv_value) * jax.nn.silu(gate_part)
    scan_out = scan_out.astype(jnp.bfloat16)
    hidden_out = (mixed.astype(jnp.float32) + jnp.dot(scan_out, w_mamba_out, preferred_element_type=jnp.float32)).astype(jnp.bfloat16)
    positions = jnp.arange(CTX, dtype=jnp.int32)
    live = (reward_mask == 1) & (positions[None, :] < lengths[:, None])
    rewards = lax.optimization_barrier(jnp.sum(jnp.where(live, reward_terms, 0.0), axis=1))
    return (hidden_out, new_key_value, new_filter_state, new_scan_state, rewards)
```

```python
import math

import jax
import jax.numpy as jnp
from jax import lax
from jax.experimental import pallas as pl
from jax.experimental.pallas import tpu as pltpu
from jax.sharding import PartitionSpec as P

EPS = 1e-06
BF16 = jnp.bfloat16
F32 = jnp.float32
Z_SIZE = 8
X_SIZE = 4


def outward(step, half):
    return half + ((step + 1) // 2) * (1 - 2 * (step % 2))


def step_kernel(
    hidden_hbm,
    gain_one_hbm,
    w_query_hbm,
    w_kv_hbm,
    w_out_hbm,
    cache_hbm,
    lengths_hbm,
    gain_two_hbm,
    w_in_hbm,
    taps_hbm,
    tap_bias_hbm,
    filter_hbm,
    w_select_hbm,
    w_step_hbm,
    step_bias_hbm,
    rate_hbm,
    skip_hbm,
    state_hbm,
    w_mamba_hbm,
    terms_hbm,
    mask_hbm,
    hidden_out,
    kv_out,
    filter_out,
    state_out,
    rewards_out,
    hidden,
    gain_one,
    w_qkv,
    w_out,
    keys,
    values,
    lengths,
    gain_two,
    w_in,
    taps,
    tap_bias,
    filters,
    w_select,
    w_step,
    step_bias,
    rate,
    skip,
    state,
    w_mamba,
    terms,
    mask,
    gathered,
    send_heads,
    got_heads,
    mixed,
    gathered_two,
    send_x,
    got_x,
    send_z,
    got_z,
    send_channels,
    got_channels,
    load_sems,
    send_sems,
    recv_sems,
):
    samples, width = hidden.shape
    heads = gathered.shape[0]
    channels = w_step.shape[1]
    rank = w_step.shape[0]
    n_state = rate.shape[0]
    me = lax.axis_index("head")
    z = me // X_SIZE
    x = me % X_SIZE

    def any_peer(i):
        dz = outward(i // X_SIZE, Z_SIZE // 2)
        dx = outward(i % X_SIZE, X_SIZE // 2)
        return ((z + dz) % Z_SIZE) * X_SIZE + (x + dx) % X_SIZE

    def x_peer(i):
        return z * X_SIZE + (x + outward(i, X_SIZE // 2)) % X_SIZE

    def z_peer(i):
        return ((z + outward(i, Z_SIZE // 2)) % Z_SIZE) * X_SIZE + x

    barrier = pltpu.get_barrier_semaphore()

    def greet(i, carry):
        pl.semaphore_signal(
            barrier, inc=1, device_id={"head": any_peer(i)}, device_id_type=pl.DeviceIdType.MESH
        )
        return carry

    lax.fori_loop(0, heads - 1, greet, 0)

    loads = []

    def load(source, target):
        copy = pltpu.make_async_copy(source, target, load_sems.at[len(loads)])
        copy.start()
        loads.append(copy)
        return copy

    load_hidden = [load(hidden_hbm, hidden), load(hidden_hbm, gathered.at[me])]
    load_qkv = [
        load(gain_one_hbm, gain_one),
        load(w_query_hbm, w_qkv.at[:, 0:width]),
        load(w_kv_hbm.at[0], w_qkv.at[:, width : 2 * width]),
        load(w_kv_hbm.at[1], w_qkv.at[:, 2 * width : 3 * width]),
    ]
    load_cache = [
        load(cache_hbm.at[0], keys),
        load(cache_hbm.at[1], values),
        load(lengths_hbm, lengths),
        load(w_out_hbm, w_out),
        load(terms_hbm, terms),
        load(mask_hbm, mask),
    ]
    load_in = [
        load(gain_two_hbm, gain_two),
        load(w_in_hbm, w_in),
        load(taps_hbm, taps),
        load(tap_bias_hbm, tap_bias),
        load(filter_hbm, filters),
        load(w_select_hbm, w_select),
    ]
    load_scan = [
        load(w_step_hbm, w_step),
        load(step_bias_hbm, step_bias),
        load(rate_hbm, rate),
        load(skip_hbm, skip),
        load(state_hbm, state),
        load(w_mamba_hbm, w_mamba),
    ]

    def wait_all(copies):
        for copy in copies:
            copy.wait()

    def send(phase, source, target, peer, count):
        def one(i, carry):
            to = peer(i)
            pltpu.make_async_remote_copy(
                src_ref=source(to),
                dst_ref=target,
                send_sem=send_sems.at[phase],
                recv_sem=recv_sems.at[phase],
                device_id={"head": to},
                device_id_type=pl.DeviceIdType.MESH,
            ).start()
            return carry

        lax.fori_loop(0, count, one, 0)

    def bytes_of(phase, buffer, count):
        part = buffer.at[pl.ds(0, count)]
        return pltpu.make_async_remote_copy(
            src_ref=part,
            dst_ref=part,
            send_sem=send_sems.at[phase],
            recv_sem=recv_sems.at[phase],
            device_id={"head": me},
            device_id_type=pl.DeviceIdType.MESH,
        )

    def normed_rows(blocks, gains):
        wide = [blocks[h].astype(F32) for h in range(heads)]
        squares = wide[0] * wide[0]
        for block in wide[1:]:
            squares = squares + block * block
        mean = jnp.sum(squares, axis=1, keepdims=True) * (1.0 / (heads * width))
        factor = lax.rsqrt(mean + EPS)
        return jnp.concatenate(
            [(wide[h] * factor * gains[h : h + 1, :]).astype(BF16) for h in range(heads)], axis=1
        )

    def summed(blocks, count):
        total = blocks[0].astype(F32)
        for h in range(1, count):
            total = total + blocks[h].astype(F32)
        return total

    wait_all(load_hidden)
    pl.semaphore_wait(barrier, heads - 1)
    send(0, lambda to: hidden, gathered.at[me], any_peer, heads - 1)
    wait_all(load_qkv)
    wait_all(load_cache)

    lane = lax.broadcasted_iota(jnp.int32, (samples, width), 1)
    row = lax.broadcasted_iota(jnp.int32, (samples, width), 0)

    def as_column(line):
        wide = jnp.concatenate([line, jnp.zeros((1, width - samples), F32)], axis=1)
        return jnp.sum(jnp.where(lane == row, wide, 0.0), axis=1, keepdims=True)

    length = as_column(lengths[...].astype(F32))
    own_columns = terms.shape[0]
    position = lax.broadcasted_iota(jnp.int32, terms.shape, 0) + me * own_columns
    live = (mask[...] == 1) & (position < lengths[...])
    reward_part = as_column(
        jnp.sum(jnp.where(live, terms[...], 0.0), axis=0, keepdims=True)
    )

    bytes_of(0, gathered, heads - 1).wait_recv()

    normed = normed_rows(gathered, gain_one)
    qkv = jnp.dot(normed, w_qkv[...], preferred_element_type=F32).astype(BF16)
    query = qkv[:, 0:width]
    new_key = qkv[:, width : 2 * width]
    new_value = qkv[:, 2 * width : 3 * width]
    kv_out[0] = new_key
    kv_out[1] = new_value
    inv_root = 1.0 / math.sqrt(width)
    context = keys.shape[0] // samples
    products = lax.dot_general(
        query, keys[...], (((1,), (1,)), ((), ())), preferred_element_type=F32
    )
    scores = products[:, 0:context]
    for b in range(1, samples):
        scores = jnp.where(row == b, products[:, b * context : (b + 1) * context], scores)
    scores = jnp.where(lane.astype(F32) < length, scores * inv_root, -jnp.inf)
    own = (
        jnp.sum(query.astype(F32) * new_key.astype(F32), axis=1, keepdims=True) * inv_root
    )
    top = jnp.maximum(jnp.max(scores, axis=1, keepdims=True), own)
    weights = jnp.exp(scores - top)
    own_weight = jnp.exp(own - top)
    total = jnp.sum(weights, axis=1, keepdims=True) + own_weight
    weights = weights / total
    own_weight = (own_weight / total).astype(BF16).astype(F32)
    placed = jnp.concatenate(
        [jnp.where(row == b, weights, 0.0).astype(BF16) for b in range(samples)], axis=1
    )
    blended = jnp.dot(placed, values[...], preferred_element_type=F32)
    attended = (blended + own_weight * new_value.astype(F32)).astype(BF16)

    head_terms = jnp.dot(attended, w_out[...], preferred_element_type=F32).astype(BF16)
    for h in range(heads):
        send_heads[h] = head_terms[:, h * width : (h + 1) * width]
    send(1, lambda to: send_heads.at[to], got_heads.at[me], any_peer, heads - 1)
    got_heads[me] = send_heads[me]
    wait_all(load_in)
    filter_sum = tap_bias[...] + filters[0] * taps[0:1, :]
    n_taps = taps.shape[0]
    for k in range(1, n_taps - 1):
        filter_sum = filter_sum + filters[k] * taps[k : k + 1, :]
    bytes_of(1, got_heads, heads - 1).wait_recv()
    mixed_block = (hidden[...].astype(F32) + summed(got_heads, heads)).astype(BF16)
    mixed[...] = mixed_block

    gathered_two[me] = mixed_block
    send(2, lambda to: mixed, gathered_two.at[me], any_peer, heads - 1)
    wait_all(load_scan)
    decay = jnp.exp(rate[...])
    bytes_of(2, gathered_two, heads - 1).wait_recv()

    normed_two = normed_rows(gathered_two, gain_two)
    x_inner = jnp.dot(normed_two, w_in[0], preferred_element_type=F32)
    conv_sum = filter_sum + x_inner * taps[n_taps - 1 : n_taps, :]
    conv_out = (conv_sum * jax.nn.sigmoid(conv_sum)).astype(BF16)
    across = (((1,), (1,)), ((), ()))
    select_low = lax.dot_general(
        conv_out, w_select[0:rank, :], across, preferred_element_type=F32
    )
    select_maps = lax.dot_general(
        conv_out, w_select[rank:, :], across, preferred_element_type=F32
    )
    n_maps = 2 * n_state
    half = width // 2

    def with_rest(block):
        high = block.astype(BF16)
        rest = block - high.astype(F32)
        return (high.astype(F32) + pltpu.roll(rest, half, 1)).astype(BF16)

    extra = jnp.concatenate(
        [select_maps, reward_part, jnp.zeros((samples, width - n_maps - 1), F32)], axis=1
    )
    packed = jnp.concatenate([select_low.astype(BF16), with_rest(extra)], axis=1)
    send_x[...] = packed
    got_x[x] = packed
    send(3, lambda to: send_x, got_x.at[x], x_peer, X_SIZE - 1)
    gate_part = jnp.dot(normed_two, w_in[1], preferred_element_type=F32)
    gate = gate_part * jax.nn.sigmoid(gate_part)
    bytes_of(3, got_x, X_SIZE - 1).wait_recv()

    def joined(total):
        low = total[:, 0:rank]
        rest = total[:, rank:]
        return low, jnp.where(lane < half, rest + pltpu.roll(rest, half, 1), 0.0)

    low, extra = joined(summed(got_x, X_SIZE))
    packed = jnp.concatenate([low.astype(BF16), with_rest(extra)], axis=1)
    send_z[...] = packed
    got_z[z] = packed
    send(4, lambda to: send_z, got_z.at[z], z_peer, Z_SIZE - 1)
    for k in range(n_taps - 2):
        filter_out[k] = filters[k + 1]
    filter_out[n_taps - 2] = x_inner
    conv_value = conv_out.astype(F32)
    skipped = skip[...] * conv_value
    bytes_of(4, got_z, Z_SIZE - 1).wait_recv()
    low, extra = joined(summed(got_z, Z_SIZE))

    pre_step = jnp.dot(low.astype(BF16), w_step[...], preferred_element_type=F32) + step_bias[...]
    step_size = jnp.maximum(pre_step, 0.0) + jnp.log1p(jnp.exp(-jnp.abs(pre_step)))
    driven = step_size * conv_value
    turned = jnp.transpose(
        jnp.concatenate([extra, jnp.zeros((width - samples, width), F32)], axis=0)
    )
    rewards_out[...] = turned[n_maps : n_maps + 1, 0:samples]
    scanned = []
    for b in range(samples):
        new_state = (
            jnp.exp(-step_size[b : b + 1, :] * decay) * state[b]
            + turned[0:n_state, b : b + 1] * driven[b : b + 1, :]
        )
        state_out[b] = new_state
        scanned.append(
            jnp.sum(turned[n_state:n_maps, b : b + 1] * new_state, axis=0, keepdims=True)
        )
    scan_out = ((jnp.concatenate(scanned, axis=0) + skipped) * gate).astype(BF16)

    channel_terms = jnp.dot(scan_out, w_mamba[...], preferred_element_type=F32).astype(BF16)
    for h in range(heads):
        send_channels[h] = channel_terms[:, h * width : (h + 1) * width]
    send(5, lambda to: send_channels.at[to], got_channels.at[me], any_peer, heads - 1)
    got_channels[me] = send_channels[me]
    for phase, buffer, count in (
        (0, gathered, heads - 1),
        (1, got_heads, heads - 1),
        (2, gathered_two, heads - 1),
        (3, got_x, X_SIZE - 1),
        (4, got_z, Z_SIZE - 1),
    ):
        bytes_of(phase, buffer, count).wait_send()
    bytes_of(5, got_channels, heads - 1).wait_recv()
    hidden_out[...] = (mixed[...].astype(F32) + summed(got_channels, heads)).astype(BF16)
    bytes_of(5, got_channels, heads - 1).wait_send()


def write_kernel(*refs):
    sems = refs[-1]
    count = (len(refs) - 1) // 2
    copies = [
        pltpu.make_async_copy(refs[i], refs[count + i], sems.at[i]) for i in range(count)
    ]
    for copy in copies:
        copy.start()
    for copy in copies:
        copy.wait()


def local(
    hidden_in,
    attention_gain,
    w_query,
    w_key_value,
    w_attention_out,
    past_cache,
    lengths,
    mamba_gain,
    w_in,
    filter_weight,
    filter_bias,
    filter_state,
    w_select,
    w_step,
    step_bias,
    log_rate,
    skip_gain,
    scan_state,
    w_mamba_out,
    reward_terms,
    reward_mask,
):
    samples, width = hidden_in.shape
    features = w_query.shape[0]
    heads = features // width
    context, head_size = past_cache.shape[3:]
    channels = w_step.shape[1]
    rank = w_step.shape[0]
    select = w_select.shape[1]
    n_taps = filter_weight.shape[0]
    n_state = log_rate.shape[0]
    lanes = -(-select // width) * width
    operands = (
        hidden_in,
        attention_gain.reshape(heads, width),
        w_query,
        w_key_value,
        w_attention_out,
        past_cache.reshape(2, samples * context, head_size),
        lengths.reshape(1, samples),
        mamba_gain.reshape(heads, width),
        w_in,
        filter_weight,
        filter_bias.reshape(1, channels),
        jnp.swapaxes(filter_state, 0, 1),
        w_select.T,
        w_step,
        step_bias.reshape(1, channels),
        log_rate,
        skip_gain.reshape(1, channels),
        scan_state,
        w_mamba_out,
        reward_terms.T,
        reward_mask.T,
    )
    scratch = [
        pltpu.VMEM((samples, width), BF16),
        pltpu.VMEM((heads, width), F32),
        pltpu.VMEM((features, 3 * width), BF16),
        pltpu.VMEM((width, features), BF16),
        pltpu.VMEM((samples * context, head_size), BF16),
        pltpu.VMEM((samples * context, head_size), BF16),
        pltpu.VMEM((1, samples), jnp.int32),
        pltpu.VMEM((heads, width), F32),
        pltpu.VMEM(w_in.shape, BF16),
        pltpu.VMEM(filter_weight.shape, F32),
        pltpu.VMEM((1, channels), F32),
        pltpu.VMEM((n_taps - 1, samples, channels), F32),
        pltpu.VMEM((select, channels), BF16),
        pltpu.VMEM(w_step.shape, BF16),
        pltpu.VMEM((1, channels), F32),
        pltpu.VMEM(log_rate.shape, F32),
        pltpu.VMEM((1, channels), F32),
        pltpu.VMEM(scan_state.shape, F32),
        pltpu.VMEM(w_mamba_out.shape, BF16),
        pltpu.VMEM(reward_terms.shape[::-1], F32),
        pltpu.VMEM(reward_mask.shape[::-1], jnp.int32),
        pltpu.VMEM((heads, samples, width), BF16),
        pltpu.VMEM((heads, samples, width), BF16),
        pltpu.VMEM((heads, samples, width), BF16),
        pltpu.VMEM((samples, width), BF16),
        pltpu.VMEM((heads, samples, width), BF16),
        pltpu.VMEM((samples, lanes), BF16),
        pltpu.VMEM((X_SIZE, samples, lanes), BF16),
        pltpu.VMEM((samples, lanes), BF16),
        pltpu.VMEM((Z_SIZE, samples, lanes), BF16),
        pltpu.VMEM((heads, samples, width), BF16),
        pltpu.VMEM((heads, samples, width), BF16),
        pltpu.SemaphoreType.DMA((24,)),
        pltpu.SemaphoreType.DMA((6,)),
        pltpu.SemaphoreType.DMA((6,)),
    ]
    vmem = pl.BlockSpec(memory_space=pltpu.VMEM)
    hbm = pl.BlockSpec(memory_space=pltpu.HBM)
    results = (
        ((samples, width), BF16),
        ((2, samples, width), BF16),
        ((n_taps - 1, samples, channels), F32),
        (scan_state.shape, F32),
        ((1, samples), F32),
    )
    found = pl.pallas_call(
        step_kernel,
        out_shape=tuple(pltpu.VMEM(shape, dtype) for shape, dtype in results),
        in_specs=[hbm] * len(operands),
        out_specs=[vmem] * len(results),
        scratch_shapes=scratch,
        compiler_params=pltpu.CompilerParams(
            collective_id=0, has_side_effects=True, vmem_limit_bytes=40 * 1024 * 1024
        ),
        name="decode_step",
    )(*(pltpu.with_memory_space_constraint(a, pltpu.HBM) for a in operands))
    hidden_out, new_kv, new_filter, new_state, rewards = pl.pallas_call(
        write_kernel,
        out_shape=tuple(pltpu.HBM(shape, dtype) for shape, dtype in results),
        in_specs=[vmem] * len(results),
        out_specs=[hbm] * len(results),
        scratch_shapes=[pltpu.SemaphoreType.DMA((len(results),))],
        compiler_params=pltpu.CompilerParams(vmem_limit_bytes=16 * 1024 * 1024),
        name="write_results",
    )(*(pltpu.with_memory_space_constraint(a, pltpu.VMEM) for a in found))
    return (
        hidden_out,
        new_kv.reshape(2, samples, 1, width),
        jnp.swapaxes(new_filter, 0, 1),
        new_state,
        rewards.reshape(samples),
    )


def solution(mesh):
    placed = (
        P("grp", "head"),
        P(),
        P(None, "head"),
        P(None, None, "head"),
        P("head", None),
        P(None, "grp", "head", None, None),
        P("grp"),
        P(),
        P(None, None, "head"),
        P(None, "head"),
        P("head"),
        P("grp", None, "head"),
        P("head", None),
        P(None, "head"),
        P("head"),
        P(None, "head"),
        P("head"),
        P("grp", None, "head"),
        P("head", None),
        P("grp", "head"),
        P("grp", "head"),
    )
    return jax.shard_map(
        local,
        mesh=mesh,
        in_specs=placed,
        out_specs=(
            P("grp", "head"),
            P(None, "grp", "head", None),
            P("grp", None, "head"),
            P("grp", None, "head"),
            P("grp"),
        ),
        check_vma=False,
    )
```

```python
import math

import jax
import jax.numpy as jnp
from jax import lax
from jax.experimental import pallas as pl
from jax.experimental.pallas import tpu as pltpu
from jax.sharding import PartitionSpec as P

EPS = 1e-06
BF16 = jnp.bfloat16
F32 = jnp.float32
Z_SIZE = 8
X_SIZE = 4


def outward(step, half):
    return half + ((step + 1) // 2) * (1 - 2 * (step % 2))


def step_kernel(
    hidden_hbm,
    gain_one_hbm,
    w_query_hbm,
    w_kv_hbm,
    w_out_hbm,
    cache_hbm,
    lengths_hbm,
    gain_two_hbm,
    w_in_hbm,
    taps_hbm,
    tap_bias_hbm,
    filter_hbm,
    w_select_hbm,
    w_step_hbm,
    step_bias_hbm,
    rate_hbm,
    skip_hbm,
    state_hbm,
    w_mamba_hbm,
    terms_hbm,
    mask_hbm,
    hidden_out,
    kv_out,
    filter_out,
    state_out,
    rewards_out,
    hidden,
    gain_one,
    w_qkv,
    w_out,
    keys,
    keys_turned,
    values,
    lengths,
    gain_two,
    w_in,
    taps,
    tap_bias,
    filters,
    w_select,
    w_step,
    step_bias,
    rate,
    skip,
    state,
    w_mamba,
    terms,
    mask,
    gathered,
    send_heads,
    got_heads,
    mixed,
    gathered_two,
    send_x,
    got_x,
    send_z,
    got_z,
    send_channels,
    got_channels,
    load_sems,
    filtered,
    arrived,
    along_x,
    along_z_sent,
    along_z,
    send_sems,
    recv_sems,
):
    samples, width = hidden.shape
    heads = gathered.shape[0]
    channels = w_step.shape[1]
    rank = w_step.shape[0]
    n_state = rate.shape[0]
    me = lax.axis_index("head")
    z = me // X_SIZE
    x = me % X_SIZE

    def x_peer(i):
        return z * X_SIZE + (x + outward(i, X_SIZE // 2)) % X_SIZE

    def z_peer(i):
        return ((z + outward(i, Z_SIZE // 2)) % Z_SIZE) * X_SIZE + x

    core = lax.axis_index("grp") % 2
    barrier = pltpu.get_barrier_semaphore()

    ring_rows = (4, 3, 5, 2, 6, 1, 7, 0)

    def row_start(dz):
        return ((z + dz) % Z_SIZE) * X_SIZE

    def in_row(dz):
        return X_SIZE if dz else X_SIZE - 1

    def hops(offset):
        dz, dx = offset
        return min(dz, Z_SIZE - dz) + min(dx, X_SIZE - dx)

    def farthest_first(rows):
        offsets = [(dz, dx) for dz in rows for dx in range(X_SIZE) if dz or dx]
        return sorted(offsets, key=hops, reverse=True)

    with jax.named_scope("greet"):
        for dz, dx in farthest_first(ring_rows):
            pl.semaphore_signal(
                barrier,
                inc=1,
                device_id={"head": row_start(dz) + (x + dx) % X_SIZE},
                device_id_type=pl.DeviceIdType.MESH,
            )

    loads = []

    def load(source, target):
        copy = pltpu.make_async_copy(source, target, load_sems.at[len(loads)])
        copy.start()
        loads.append(copy)
        return copy

    load_hidden = [load(hidden_hbm, hidden), load(hidden_hbm, gathered.at[me])]
    load_qkv = [
        load(gain_one_hbm, gain_one),
        load(w_query_hbm, w_qkv.at[:, 0:width]),
        load(w_kv_hbm.at[0], w_qkv.at[:, width : 2 * width]),
        load(w_kv_hbm.at[1], w_qkv.at[:, 2 * width : 3 * width]),
    ]
    load_cache = [
        load(cache_hbm.at[0], keys),
        load(cache_hbm.at[1], values),
        load(lengths_hbm, lengths),
        load(w_out_hbm, w_out),
        load(terms_hbm, terms),
        load(mask_hbm, mask),
    ]
    load_in = [
        load(gain_two_hbm, gain_two),
        load(w_in_hbm, w_in),
        load(taps_hbm, taps),
        load(tap_bias_hbm, tap_bias),
        load(filter_hbm, filters),
        load(w_select_hbm, w_select),
    ]
    load_scan = [
        load(w_step_hbm, w_step),
        load(step_bias_hbm, step_bias),
        load(rate_hbm, rate),
        load(skip_hbm, skip),
        load(state_hbm, state),
        load(w_mamba_hbm, w_mamba),
    ]

    def wait_all(copies):
        for copy in copies:
            copy.wait()

    def send(phase, source, target, peer, first, last):
        def one(i, carry):
            to = peer(i)
            pltpu.make_async_remote_copy(
                src_ref=source(to),
                dst_ref=target,
                send_sem=send_sems.at[phase],
                recv_sem=recv_sems.at[phase],
                device_id={"head": to},
                device_id_type=pl.DeviceIdType.MESH,
            ).start()
            return carry

        lax.fori_loop(first, last, one, 0)

    def bytes_of(phase, buffer, count):
        part = buffer.at[pl.ds(0, count)]
        return pltpu.make_async_remote_copy(
            src_ref=part,
            dst_ref=part,
            send_sem=send_sems.at[phase],
            recv_sem=recv_sems.at[phase],
            device_id={"head": me},
            device_id_type=pl.DeviceIdType.MESH,
        )

    def send_to(offset, sem, source, target):
        dz, dx = offset
        to = row_start(dz) + (x + dx) % X_SIZE
        pltpu.make_async_remote_copy(
            src_ref=source(to),
            dst_ref=target,
            send_sem=send_sems.at[sem],
            recv_sem=recv_sems.at[sem],
            device_id={"head": to},
            device_id_type=pl.DeviceIdType.MESH,
        ).start()

    def gather(sem, source, target):
        for offset in farthest_first(ring_rows):
            send_to(offset, sem + offset[0], lambda to: source, target)

    depth = X_SIZE * width

    def row_at(first):
        return pl.ds(pl.multiple_of(first * width, depth), depth)

    def scaled_row(first, blocks, gains):
        wide = [blocks[first + k].astype(F32) for k in range(X_SIZE)]
        scale = gains[pl.ds(first, X_SIZE), :]
        scaled = [(wide[k] * scale[k : k + 1, :]).astype(BF16) for k in range(X_SIZE)]
        return wide, jnp.concatenate(scaled, axis=1)

    def projected_rows(sem, blocks, gains, weights):
        squares = jnp.zeros((samples, width), F32)
        total = jnp.zeros((samples, weights(pl.ds(0, depth)).shape[1]), F32)
        for dz in ring_rows:
            first = row_start(Z_SIZE - dz)
            with jax.named_scope("wait_row"):
                bytes_of(sem + dz, blocks, in_row(dz)).wait_recv()
            wide, scaled = scaled_row(first, blocks, gains)
            for block in wide:
                squares = squares + block * block
            total = total + jnp.dot(
                scaled, weights(row_at(first)), preferred_element_type=F32
            )
        return squares, total

    def place_terms(rows, weights, sent, some_rows):
        for dz in some_rows:
            first = row_start(dz)
            part = jnp.dot(
                rows, weights[:, row_at(first)], preferred_element_type=F32
            ).astype(BF16)
            for k in range(X_SIZE):
                sent[first // X_SIZE, k] = part[:, k * width : (k + 1) * width]

    def scatter_sums(sem, rows, weights, sent, landed, result, meanwhile):
        @pl.when(core == 0)
        def _():
            for half in (ring_rows[:4], ring_rows[4:]):
                place_terms(rows, weights, sent, half)
                for offset in farthest_first(half):
                    send_to(
                        offset,
                        sem,
                        lambda to: sent.at[to // X_SIZE, to % X_SIZE],
                        landed.at[me],
                    )
            landed[me] = sent[z, x]

        @pl.when(core == 1)
        def _():
            place_terms(rows, weights, sent, ring_rows)
            send(sem + 1, lambda to: sent.at[:, to % X_SIZE], along_x.at[x], x_peer, 0, X_SIZE - 1)
            along_x[x] = sent[:, x]

        meanwhile()

        @pl.when(core == 0)
        def _():
            bytes_of(sem, landed, heads - 1).wait_recv()
            result[...] = summed(landed, heads)

        @pl.when(core == 1)
        def _():
            bytes_of(sem + 1, along_x, X_SIZE - 1).wait_recv()
            part = summed(along_x, X_SIZE).astype(BF16)
            along_z_sent[...] = part
            send(
                sem + 2, lambda to: along_z_sent.at[to // X_SIZE], along_z.at[z], z_peer, 0, Z_SIZE - 1
            )
            along_z[z] = along_z_sent[z]
            bytes_of(sem + 1, along_x, X_SIZE - 1).wait_send()
            bytes_of(sem + 2, along_z, Z_SIZE - 1).wait_recv()
            result[...] = summed(along_z, Z_SIZE)
            bytes_of(sem + 2, along_z, Z_SIZE - 1).wait_send()

    def scatter_direct(sem, rows, weights, sent, landed, result, meanwhile):
        for half in (ring_rows[:4], ring_rows[4:]):
            place_terms(rows, weights, sent, half)
            for offset in farthest_first(half):
                send_to(
                    offset,
                    sem,
                    lambda to: sent.at[to // X_SIZE, to % X_SIZE],
                    landed.at[me],
                )
        landed[me] = sent[z, x]
        meanwhile()
        bytes_of(sem, landed, heads - 1).wait_recv()
        result[...] = summed(landed, heads)

    def row_factor(squares):
        mean = jnp.sum(squares, axis=1, keepdims=True) * (1.0 / (heads * width))
        return lax.rsqrt(mean + EPS)

    def summed(blocks, count):
        total = blocks[0].astype(F32)
        for h in range(1, count):
            total = total + blocks[h].astype(F32)
        return total

    wait_all(load_hidden)
    pl.semaphore_wait(barrier, heads - 1)
    with jax.named_scope("send_rows"):
        gather(0, hidden, gathered.at[me])
    wait_all(load_qkv)
    wait_all(load_cache)

    lane = lax.broadcasted_iota(jnp.int32, (samples, width), 1)
    row = lax.broadcasted_iota(jnp.int32, (samples, width), 0)

    def as_column(line):
        wide = jnp.concatenate([line, jnp.zeros((1, width - samples), F32)], axis=1)
        return jnp.sum(jnp.where(lane == row, wide, 0.0), axis=1, keepdims=True)

    length = as_column(lengths[...].astype(F32))
    own_columns = terms.shape[0]
    position = lax.broadcasted_iota(jnp.int32, terms.shape, 0) + me * own_columns
    live = (mask[...] == 1) & (position < lengths[...])
    reward_part = as_column(
        jnp.sum(jnp.where(live, terms[...], 0.0), axis=0, keepdims=True)
    )

    with jax.named_scope("turn_keys"):
        keys_turned[...] = jnp.transpose(keys[...])

    with jax.named_scope("rows"):
        squares, product = projected_rows(0, gathered, gain_one, lambda at: w_qkv[at, :])
    with jax.named_scope("attend"):
        qkv = (product * row_factor(squares)).astype(BF16)
        query = qkv[:, 0:width]
        new_key = qkv[:, width : 2 * width]
        new_value = qkv[:, 2 * width : 3 * width]
    with jax.named_scope("scores"):
        inv_root = 1.0 / math.sqrt(width)
        context = keys.shape[0] // samples
        products = jnp.dot(query, keys_turned[...], preferred_element_type=F32)
        scores = products[:, 0:context]
        for b in range(1, samples):
            scores = jnp.where(row == b, products[:, b * context : (b + 1) * context], scores)
    with jax.named_scope("softmax"):
        scores = jnp.where(lane.astype(F32) < length, scores * inv_root, -jnp.inf)
        own = (
            jnp.sum(query.astype(F32) * new_key.astype(F32), axis=1, keepdims=True) * inv_root
        )
        top = jnp.maximum(jnp.max(scores, axis=1, keepdims=True), own)
        weights = jnp.exp(scores - top)
        own_weight = jnp.exp(own - top)
        total = jnp.sum(weights, axis=1, keepdims=True) + own_weight
        inverse = 1.0 / total
    with jax.named_scope("blend"):
        placed = jnp.concatenate(
            [jnp.where(row == b, weights, 0.0).astype(BF16) for b in range(samples)], axis=1
        )
        blended = jnp.dot(placed, values[...], preferred_element_type=F32)
        attended = ((blended + own_weight * new_value.astype(F32)) * inverse).astype(BF16)

    n_taps = taps.shape[0]

    def while_heads_travel():
        kv_out[0] = new_key
        kv_out[1] = new_value
        wait_all(load_in)
        filter_sum = tap_bias[...] + filters[0] * taps[0:1, :]
        for k in range(1, n_taps - 1):
            filter_sum = filter_sum + filters[k] * taps[k : k + 1, :]
        filtered[...] = filter_sum

    with jax.named_scope("head_terms"):
        scatter_direct(
            8, attended, w_out, send_heads, got_heads, arrived, while_heads_travel
        )
    with jax.named_scope("sum_heads"):
        mixed_block = (hidden[...].astype(F32) + arrived[...]).astype(BF16)
        mixed[...] = mixed_block

    with jax.named_scope("send_mixed"):
        gather(9, mixed, gathered_two.at[me])
    gathered_two[me] = mixed_block
    wait_all(load_scan)
    decay = jnp.exp(rate[...])
    with jax.named_scope("mixed_rows"):
        squares, product = projected_rows(9, gathered_two, gain_two, lambda at: w_in[0, at, :])
        factor_two = row_factor(squares)
        x_inner = product * factor_two
    with jax.named_scope("select"):
        conv_sum = filtered[...] + x_inner * taps[n_taps - 1 : n_taps, :]
        conv_out = (conv_sum * jax.nn.sigmoid(conv_sum)).astype(BF16)
        selected = lax.dot_general(
            conv_out, w_select[...], (((1,), (1,)), ((), ())), preferred_element_type=F32
        )
        n_maps = 2 * n_state
        group = 8
        stride = n_maps + group
        at_lane = lax.broadcasted_iota(jnp.int32, (group, width), 1)
        high_place = (at_lane == n_maps) | (at_lane == n_maps + stride) | (
            at_lane == n_maps + 2 * stride
        )
        low_place = (at_lane == n_maps + 1) | (at_lane == n_maps + 1 + stride) | (
            at_lane == n_maps + 1 + 2 * stride
        )

        def payload(low, extra):
            rounded = extra.astype(BF16).astype(F32)
            rest = pltpu.roll(extra - rounded, 1, 1)
            extra = jnp.where(low_place, rest, extra)
            return jnp.concatenate(
                [low[:, 0:width], low[:, width : 2 * width], extra], axis=0
            ).astype(BF16)

        def opened(total):
            low = jnp.concatenate([total[0:samples], total[samples : 2 * samples]], axis=1)
            extra = total[2 * samples :]
            extra = jnp.where(high_place, extra + pltpu.roll(extra, width - 1, 1), extra)
            return low, extra

        wide = jnp.concatenate(
            [selected[:, rank:], reward_part, jnp.zeros((samples, width - n_maps - 1), F32)],
            axis=1,
        )
        extra = (
            wide[0:group]
            + pltpu.roll(wide[group : 2 * group], stride, 1)
            + pltpu.roll(wide[2 * group : 3 * group], 2 * stride, 1)
        )
        packed = payload(selected[:, 0:rank], extra)
        send_x[...] = packed
    with jax.named_scope("send_x"):
        send(17, lambda to: send_x, got_x.at[x], x_peer, 0, X_SIZE - 1)
    got_x[x] = packed
    with jax.named_scope("gate"):
        gate_parts = jnp.zeros((samples, channels), F32)
        for dz in ring_rows:
            first = row_start(dz)
            _, scaled = scaled_row(first, gathered_two, gain_two)
            gate_parts = gate_parts + jnp.dot(
                scaled, w_in[1, row_at(first), :], preferred_element_type=F32
            )
        gate_part = gate_parts * factor_two
        gate = gate_part * jax.nn.sigmoid(gate_part)
    with jax.named_scope("wait_x"):
        bytes_of(17, got_x, X_SIZE - 1).wait_recv()
    with jax.named_scope("sum_x"):
        low, extra = opened(summed(got_x, X_SIZE))
        packed = payload(low, extra)
        send_z[...] = packed
    with jax.named_scope("send_z"):
        send(18, lambda to: send_z, got_z.at[z], z_peer, 0, Z_SIZE - 1)
    got_z[z] = packed
    for k in range(n_taps - 2):
        filter_out[k] = filters[k + 1]
    filter_out[n_taps - 2] = x_inner
    conv_value = conv_out.astype(F32)
    skipped = skip[...] * conv_value
    with jax.named_scope("wait_z"):
        bytes_of(18, got_z, Z_SIZE - 1).wait_recv()

    with jax.named_scope("step_size"):
        low, extra = opened(summed(got_z, Z_SIZE))
        pre_step = (
            jnp.dot(low.astype(BF16), w_step[...], preferred_element_type=F32) + step_bias[...]
        )
        step_size = jnp.maximum(pre_step, 0.0) + jnp.log1p(jnp.exp(-jnp.abs(pre_step)))
        driven = step_size * conv_value
        turned = jnp.transpose(
            jnp.concatenate([extra, jnp.zeros((width - group, width), F32)], axis=0)
        )
    with jax.named_scope("scan"):
        scanned = []
        for b in range(samples):
            base, column = (b // group) * stride, b % group
            into = turned[base : base + n_state, column : column + 1]
            out_of = turned[base + n_state : base + n_maps, column : column + 1]
            new_state = (
                jnp.exp(-step_size[b : b + 1, :] * decay) * state[b]
                + into * driven[b : b + 1, :]
            )
            state_out[b] = new_state
            scanned.append(jnp.sum(out_of * new_state, axis=0, keepdims=True))
        scan_out = ((jnp.concatenate(scanned, axis=0) + skipped) * gate).astype(BF16)


    def while_channels_travel():
        rewards_out[...] = jnp.concatenate(
            [
                turned[k * stride + n_maps : k * stride + n_maps + 1, 0:group]
                for k in range(samples // group)
            ],
            axis=1,
        )
        for dz in ring_rows:
            bytes_of(dz, gathered, in_row(dz)).wait_send()
            bytes_of(9 + dz, gathered_two, in_row(dz)).wait_send()
        bytes_of(8, got_heads, heads - 1).wait_send()
        bytes_of(17, got_x, X_SIZE - 1).wait_send()
        bytes_of(18, got_z, Z_SIZE - 1).wait_send()

    with jax.named_scope("channel_terms"):
        scatter_sums(
            19, scan_out, w_mamba, send_channels, got_channels, arrived, while_channels_travel
        )
    hidden_out[...] = (mixed[...].astype(F32) + arrived[...]).astype(BF16)

    @pl.when(core == 0)
    def _():
        bytes_of(19, got_channels, heads - 1).wait_send()


def write_kernel(*refs):
    sems = refs[-1]
    count = (len(refs) - 1) // 2
    copies = [
        pltpu.make_async_copy(refs[i], refs[count + i], sems.at[i]) for i in range(count)
    ]
    for copy in copies:
        copy.start()
    for copy in copies:
        copy.wait()


def local(
    hidden_in,
    attention_gain,
    w_query,
    w_key_value,
    w_attention_out,
    past_cache,
    lengths,
    mamba_gain,
    w_in,
    filter_weight,
    filter_bias,
    filter_state,
    w_select,
    w_step,
    step_bias,
    log_rate,
    skip_gain,
    scan_state,
    w_mamba_out,
    reward_terms,
    reward_mask,
):
    samples, width = hidden_in.shape
    features = w_query.shape[0]
    heads = features // width
    context, head_size = past_cache.shape[3:]
    channels = w_step.shape[1]
    rank = w_step.shape[0]
    select = w_select.shape[1]
    n_taps = filter_weight.shape[0]
    n_state = log_rate.shape[0]
    packed = 2 * samples + 8
    operands = (
        hidden_in,
        attention_gain.reshape(heads, width),
        w_query,
        w_key_value,
        w_attention_out,
        past_cache.reshape(2, samples * context, head_size),
        lengths.reshape(1, samples),
        mamba_gain.reshape(heads, width),
        w_in,
        filter_weight,
        filter_bias.reshape(1, channels),
        jnp.swapaxes(filter_state, 0, 1),
        w_select.T,
        w_step,
        step_bias.reshape(1, channels),
        log_rate,
        skip_gain.reshape(1, channels),
        scan_state,
        w_mamba_out,
        reward_terms.T,
        reward_mask.T,
    )
    scratch = [
        pltpu.VMEM((samples, width), BF16),
        pltpu.VMEM((heads, width), F32),
        pltpu.VMEM((features, 3 * width), BF16),
        pltpu.VMEM((width, features), BF16),
        pltpu.VMEM((samples * context, head_size), BF16),
        pltpu.VMEM((head_size, samples * context), BF16),
        pltpu.VMEM((samples * context, head_size), BF16),
        pltpu.VMEM((1, samples), jnp.int32),
        pltpu.VMEM((heads, width), F32),
        pltpu.VMEM(w_in.shape, BF16),
        pltpu.VMEM(filter_weight.shape, F32),
        pltpu.VMEM((1, channels), F32),
        pltpu.VMEM((n_taps - 1, samples, channels), F32),
        pltpu.VMEM((select, channels), BF16),
        pltpu.VMEM(w_step.shape, BF16),
        pltpu.VMEM((1, channels), F32),
        pltpu.VMEM(log_rate.shape, F32),
        pltpu.VMEM((1, channels), F32),
        pltpu.VMEM(scan_state.shape, F32),
        pltpu.VMEM(w_mamba_out.shape, BF16),
        pltpu.VMEM(reward_terms.shape[::-1], F32),
        pltpu.VMEM(reward_mask.shape[::-1], jnp.int32),
        pltpu.VMEM((heads, samples, width), BF16),
        pltpu.VMEM((Z_SIZE, X_SIZE, samples, width), BF16),
        pltpu.VMEM((heads, samples, width), BF16),
        pltpu.VMEM((samples, width), BF16),
        pltpu.VMEM((heads, samples, width), BF16),
        pltpu.VMEM((packed, width), BF16),
        pltpu.VMEM((X_SIZE, packed, width), BF16),
        pltpu.VMEM((packed, width), BF16),
        pltpu.VMEM((Z_SIZE, packed, width), BF16),
        pltpu.VMEM((Z_SIZE, X_SIZE, samples, width), BF16),
        pltpu.VMEM((heads, samples, width), BF16),
        pltpu.SemaphoreType.DMA((24,)),
        pltpu.VMEM((samples, channels), F32),
        pltpu.VMEM((samples, width), F32),
        pltpu.VMEM((X_SIZE, Z_SIZE, samples, width), BF16),
        pltpu.VMEM((Z_SIZE, samples, width), BF16),
        pltpu.VMEM((Z_SIZE, samples, width), BF16),
        pltpu.SemaphoreType.DMA((27,)),
        pltpu.SemaphoreType.DMA((27,)),
    ]
    vmem = pl.BlockSpec(memory_space=pltpu.VMEM)
    hbm = pl.BlockSpec(memory_space=pltpu.HBM)
    results = (
        ((samples, width), BF16),
        ((2, samples, width), BF16),
        ((n_taps - 1, samples, channels), F32),
        (scan_state.shape, F32),
        ((1, samples), F32),
    )
    found = pl.pallas_call(
        step_kernel,
        out_shape=tuple(pltpu.VMEM(shape, dtype) for shape, dtype in results),
        in_specs=[hbm] * len(operands),
        out_specs=[vmem] * len(results),
        scratch_shapes=scratch,
        compiler_params=pltpu.CompilerParams(
            collective_id=0, has_side_effects=True, vmem_limit_bytes=40 * 1024 * 1024
        ),
        name="decode_step",
    )(*(pltpu.with_memory_space_constraint(a, pltpu.HBM) for a in operands))
    hidden_out, new_kv, new_filter, new_state, rewards = pl.pallas_call(
        write_kernel,
        out_shape=tuple(pltpu.HBM(shape, dtype) for shape, dtype in results),
        in_specs=[vmem] * len(results),
        out_specs=[hbm] * len(results),
        scratch_shapes=[pltpu.SemaphoreType.DMA((len(results),))],
        compiler_params=pltpu.CompilerParams(vmem_limit_bytes=16 * 1024 * 1024),
        name="write_results",
    )(*(pltpu.with_memory_space_constraint(a, pltpu.VMEM) for a in found))
    return (
        hidden_out,
        new_kv.reshape(2, samples, 1, width),
        jnp.swapaxes(new_filter, 0, 1),
        new_state,
        rewards.reshape(samples),
    )


def solution(mesh):
    placed = (
        P("grp", "head"),
        P(),
        P(None, "head"),
        P(None, None, "head"),
        P("head", None),
        P(None, "grp", "head", None, None),
        P("grp"),
        P(),
        P(None, None, "head"),
        P(None, "head"),
        P("head"),
        P("grp", None, "head"),
        P("head", None),
        P(None, "head"),
        P("head"),
        P(None, "head"),
        P("head"),
        P("grp", None, "head"),
        P("head", None),
        P("grp", "head"),
        P("grp", "head"),
    )
    return jax.shard_map(
        local,
        mesh=mesh,
        in_specs=placed,
        out_specs=(
            P("grp", "head"),
            P(None, "grp", "head", None),
            P("grp", None, "head"),
            P("grp", None, "head"),
            P("grp"),
        ),
        check_vma=False,
    )
```
